16 devices in a mesh: data: 2 (over y, z), dap: 8 (over x, core).
Axes of the slice: x: 4, y: 2, z: 1, core: 2. Of those that a mesh axis runs over, the one named last changes fastest.
The devices are a block of a 4x4x8 slice.
Arguments:
- pair_rep: bfloat16 [16, 384, 384, 128], P('data', 'dap'), parts along dimension 0
- pair_mask: int32 [16, 384, 384], P('data', 'dap'), parts along dimension 0
- norm_gain: bfloat16 [2, 128], replicated
- norm_bias: bfloat16 [2, 128], replicated
- w_proj: bfloat16 [2, 128, 512], replicated
- w_gate: bfloat16 [2, 128, 128], replicated
- hid_gain: bfloat16 [2, 128], replicated
- hid_bias: bfloat16 [2, 128], replicated
- w_out: bfloat16 [2, 128, 128], replicated
Outputs:
- output: bfloat16 [16, 384, 384, 128], P('data', None, 'dap'), parts along dimension 0
There are 2 independent parts. The reference program is written for one: setup_inputs(seed, part) draws one part's arguments, and reference() takes and returns one part's arrays. A program takes and returns all parts, laid end to end along the dimension named above; an argument that names none is the same for every part.
All inputs are finite; a program needn't handle non-finite values.
Results may differ from the reference program's by a relative error of at most 0.00597921.
Values are sent between devices in bfloat16 or wider.
A program may use at most 768 MiB of HBM per device.

```python
import jax
import jax.numpy as jnp
from jax import lax

NUM_CROPS = 8
N_RES = 384
C_PAIR = 128
C_HIDDEN = 128
LN_EPS = 1e-5
BLOCK_ROWS = min(N_RES, 64)


def setup_inputs(seed: int = 0, part: int = 0) -> dict:
    key_list = jax.random.split(jax.random.key(seed), 8)
    part_key = jax.random.fold_in(key_list[0], part)
    key_pair, key_keep, key_len = jax.random.split(part_key, 3)
    pair_vals = jax.random.normal(key_pair, (NUM_CROPS, N_RES, N_RES, C_PAIR), jnp.float32)
    keep_res = jax.random.randint(key_keep, (NUM_CROPS, N_RES), 0, 16) != 0
    pad_len = jax.random.randint(key_len, (NUM_CROPS, 1), 0, N_RES // 8 + 1)
    res_valid = (keep_res & (jnp.arange(N_RES)[None, :] < N_RES - pad_len)).astype(jnp.int32)
    pair_mask = res_valid[:, :, None] * res_valid[:, None, :]
    norm_gain = 1.0 + 0.3 * jax.random.normal(key_list[1], (2, C_PAIR), jnp.float32)
    norm_bias = 0.3 * jax.random.normal(key_list[2], (2, C_PAIR), jnp.float32)
    w_proj = jax.random.normal(key_list[3], (2, C_PAIR, 4 * C_HIDDEN), jnp.float32) * C_PAIR ** -0.5
    w_gate = jax.random.normal(key_list[4], (2, C_PAIR, C_PAIR), jnp.float32) * C_PAIR ** -0.5
    hid_gain = 1.0 + 0.3 * jax.random.normal(key_list[5], (2, C_HIDDEN), jnp.float32)
    hid_bias = 0.3 * jax.random.normal(key_list[6], (2, C_HIDDEN), jnp.float32)
    w_out = jax.random.normal(key_list[7], (2, C_HIDDEN, C_PAIR), jnp.float32) * C_HIDDEN ** -0.5
    return {
        'pair_rep': pair_vals.astype(jnp.bfloat16),
        'pair_mask': pair_mask,
        'norm_gain': norm_gain.astype(jnp.bfloat16),
        'norm_bias': norm_bias.astype(jnp.bfloat16),
        'w_proj': w_proj.astype(jnp.bfloat16),
        'w_gate': w_gate.astype(jnp.bfloat16),
        'hid_gain': hid_gain.astype(jnp.bfloat16),
        'hid_bias': hid_bias.astype(jnp.bfloat16),
        'w_out': w_out.astype(jnp.bfloat16),
    }


def layer_norm(values, gain_vec, bias_vec):
    centred = values - jnp.mean(values, axis=-1, keepdims=True)
    var_val = jnp.mean(centred * centred, axis=-1, keepdims=True)
    return centred * lax.rsqrt(var_val + LN_EPS) * gain_vec.astype(jnp.float32) + bias_vec.astype(jnp.float32)


def project(pair_rows, mask_rows, norm_gain, norm_bias, w_proj):
    normed = layer_norm(pair_rows.astype(jnp.float32), norm_gain, norm_bias).astype(jnp.bfloat16)
    proj_all = jnp.dot(normed.reshape(-1, C_PAIR), w_proj, preferred_element_type=jnp.float32)
    proj_all = proj_all.reshape(BLOCK_ROWS, N_RES, 4, C_HIDDEN)
    mask_f = mask_rows.astype(jnp.float32)[:, :, None]
    left_proj = (mask_f * jax.nn.sigmoid(proj_all[:, :, 1]) * proj_all[:, :, 0]).astype(jnp.bfloat16)
    right_proj = (mask_f * jax.nn.sigmoid(proj_all[:, :, 3]) * proj_all[:, :, 2]).astype(jnp.bfloat16)
    return left_proj, right_proj


def finish(pair_rows, tri_sum, norm_gain, norm_bias, w_gate, hid_gain, hid_bias, w_out):
    normed = layer_norm(pair_rows.astype(jnp.float32), norm_gain, norm_bias).astype(jnp.bfloat16)
    gate_val = jax.nn.sigmoid(jnp.dot(normed.reshape(-1, C_PAIR), w_gate, preferred_element_type=jnp.float32))
    tri_round = tri_sum.astype(jnp.bfloat16).astype(jnp.float32)
    hid_norm = layer_norm(tri_round, hid_gain, hid_bias).astype(jnp.bfloat16)
    out_proj = jnp.dot(hid_norm.reshape(-1, C_HIDDEN), w_out, preferred_element_type=jnp.float32)
    new_rows = pair_rows.astype(jnp.float32) + (gate_val * out_proj).reshape(BLOCK_ROWS, N_RES, C_PAIR)
    return new_rows.astype(jnp.bfloat16)


def tri_update(pair_grid, mask_grid, weights, layer_idx, incoming):
    norm_gain, norm_bias, w_proj, w_gate, hid_gain, hid_bias, w_out = [w_arr[layer_idx] for w_arr in weights]
    n_blocks = N_RES // BLOCK_ROWS

    def proj_block(blk_idx):
        row_start = blk_idx * BLOCK_ROWS
        pair_rows = lax.dynamic_slice_in_dim(pair_grid, row_start, BLOCK_ROWS, 0)
        mask_rows = lax.dynamic_slice_in_dim(mask_grid, row_start, BLOCK_ROWS, 0)
        return project(pair_rows, mask_rows, norm_gain, norm_bias, w_proj)

    left_proj, right_proj = lax.map(proj_block, jnp.arange(n_blocks))
    left_proj = left_proj.reshape(N_RES, N_RES, C_HIDDEN)
    right_all = right_proj.reshape(N_RES, N_RES, C_HIDDEN).astype(jnp.float32)

    def out_block(blk_idx):
        row_start = blk_idx * BLOCK_ROWS
        pair_rows = lax.dynamic_slice_in_dim(pair_grid, row_start, BLOCK_ROWS, 0)
        if incoming:
            left_blk = lax.dynamic_slice_in_dim(left_proj, row_start, BLOCK_ROWS, 1).astype(jnp.float32)
            tri_sum = jnp.einsum('kic,kjc->ijc', left_blk, right_all)
        else:
            left_blk = lax.dynamic_slice_in_dim(left_proj, row_start, BLOCK_ROWS, 0).astype(jnp.float32)
            tri_sum = jnp.einsum('ikc,jkc->ijc', left_blk, right_all)
        return finish(pair_rows, tri_sum, norm_gain, norm_bias, w_gate, hid_gain, hid_bias, w_out)

    new_grid = lax.map(out_block, jnp.arange(n_blocks))
    return new_grid.reshape(N_RES, N_RES, C_PAIR)


def reference(pair_rep, pair_mask, norm_gain, norm_bias, w_proj, w_gate, hid_gain, hid_bias, w_out):
    weights = (norm_gain, norm_bias, w_proj, w_gate, hid_gain, hid_bias, w_out)

    def per_crop(crop_item):
        pair_grid, mask_grid = crop_item
        mid_grid = tri_update(pair_grid, mask_grid, weights, 0, False)
        return tri_update(mid_grid, mask_grid, weights, 1, True)

    return lax.map(per_crop, (pair_rep, pair_mask))
```

```python
import functools, jax, jax.numpy as jnp
from jax import lax
from jax.experimental import pallas as pl
from jax.experimental.pallas import tpu as pltpu
from jax.sharding import PartitionSpec as P


EPS = 1e-5
AHEAD = 2
BF = jnp.bfloat16
F32 = jnp.float32

def ln_cols(v, g, b):
    mu = jnp.mean(v, axis=0, keepdims=True)
    cen = v - mu
    var = jnp.mean(cen * cen, axis=0, keepdims=True)
    return cen * lax.rsqrt(var + EPS) * g + b

def gated(p, g, half_mask):
    return (p * half_mask) * (1.0 + jnp.tanh(0.5 * g))

def k1_body(nsplit, s_ref, z_ref, m_ref, w_ref, g_ref, b_ref, *rest):
    outs, scr, ms = rest[:nsplit], rest[nsplit:-1], rest[-1]
    ch = g_ref.shape[0]
    ms[...] = 0.5 * m_ref[...].astype(F32)
    def row(r, _):
        x = ln_cols(z_ref[r].astype(F32), g_ref[...], b_ref[...]).astype(BF)
        hm = ms[pl.ds(r, 1), :]
        q = jnp.dot(w_ref[...], x, preferred_element_type=F32)
        for s in range(nsplit):
            p = q[2 * s * ch:(2 * s + 1) * ch]
            g = q[(2 * s + 1) * ch:(2 * s + 2) * ch]
            scr[s][r] = gated(p, g, hm).astype(BF)
        return 0
    lax.fori_loop(0, z_ref.shape[0], row, 0, unroll=2)
    for s in range(nsplit):
        outs[s][...] = jnp.swapaxes(scr[s][...], 0, 1)

def proj(z, m, h, nblk, w_t, g, b, nsplit, rows=16):
    C, N = z.shape[1], z.shape[2]
    ch = C
    return pl.pallas_call(
        functools.partial(k1_body, nsplit),
        grid_spec=pltpu.PrefetchScalarGridSpec(
            num_scalar_prefetch=1, grid=(nblk,),
            in_specs=[pl.BlockSpec((rows, C, N), lambda i, s: (s[0] * nblk + i, 0, 0)),
                      pl.BlockSpec((rows, N), lambda i, s: (s[0] * nblk + i, 0)),
                      pl.BlockSpec(w_t.shape, lambda i, s: (0, 0)),
                      pl.BlockSpec(g.shape, lambda i, s: (0, 0)),
                      pl.BlockSpec(b.shape, lambda i, s: (0, 0))],
            out_specs=[pl.BlockSpec((ch, rows, N), lambda i, s: (0, i, 0))] * nsplit,
            scratch_shapes=[pltpu.VMEM((rows, ch, N), BF)] * nsplit + [pltpu.VMEM((rows, N), F32)]),
        out_shape=[jax.ShapeDtypeStruct((ch, nblk * rows, N), BF)] * nsplit,
        cost_estimate=pl.CostEstimate(flops=nblk * rows * N * C * 2 * C * 2 * nsplit * 4, bytes_accessed=nblk * rows * N * C * 2 * (1 + nsplit), transcendentals=0),
        name="proj",
    )(h, z, m, w_t, g, b)

def tri0_body(s_ref, a_ref, bo_ref, bp_ref, t_ref, bs):
    half = bo_ref.shape[1]
    h = s_ref[0]
    o0 = pl.multiple_of(h * half, 16)
    o1 = pl.multiple_of((1 - h) * half, 16)
    bs[:, pl.ds(o0, half), :] = bo_ref[...]
    bs[:, pl.ds(o1, half), :] = bp_ref[...]
    def one(c, _):
        t_ref[c] = lax.dot_general(a_ref[c], bs[c], (((1,), (1,)), ((), ())), preferred_element_type=F32).astype(BF)
        return 0
    lax.fori_loop(0, a_ref.shape[0], one, 0, unroll=2)

def tri0(h, a, bo, bp, cb=8):
    C, R, N = a.shape
    H = bo.shape[1]
    return pl.pallas_call(
        tri0_body,
        grid_spec=pltpu.PrefetchScalarGridSpec(
            num_scalar_prefetch=1, grid=(C // cb,),
            in_specs=[pl.BlockSpec((cb, R, N), lambda i, s: (i, 0, 0)),
                      pl.BlockSpec((cb, H, N), lambda i, s: (i, 0, 0)),
                      pl.BlockSpec((cb, H, N), lambda i, s: (i, 0, 0))],
            out_specs=pl.BlockSpec((cb, R, 2 * H), lambda i, s: (i, 0, 0)),
            scratch_shapes=[pltpu.VMEM((cb, 2 * H, N), BF)]),
        out_shape=jax.ShapeDtypeStruct((C, R, 2 * H), BF),
        cost_estimate=pl.CostEstimate(flops=C * R * N * 2 * H * 2, bytes_accessed=2 * C * N * (2 * R + 2 * H), transcendentals=0),
        name="tri0",
    )(h, a, bo, bp)

def tri1_body(s_ref, b_ref, ao_ref, ap_ref, t_ref, asc):
    half = ao_ref.shape[1]
    h = s_ref[0]
    o0 = pl.multiple_of(h * half, 16)
    o1 = pl.multiple_of((1 - h) * half, 16)
    asc[:, pl.ds(o0, half), :] = ao_ref[...]
    asc[:, pl.ds(o1, half), :] = ap_ref[...]
    def one(c, _):
        t_ref[c] = jnp.dot(b_ref[c], asc[c], preferred_element_type=F32).astype(BF)
        return 0
    lax.fori_loop(0, b_ref.shape[0], one, 0, unroll=2)

def tri1(h, b, ao, ap, cb=8):
    C, J, K = b.shape
    H, N = ao.shape[1:]
    return pl.pallas_call(
        tri1_body,
        grid_spec=pltpu.PrefetchScalarGridSpec(
            num_scalar_prefetch=1, grid=(C // cb,),
            in_specs=[pl.BlockSpec((cb, J, K), lambda i, s: (i, 0, 0)),
                      pl.BlockSpec((cb, H, N), lambda i, s: (i, 0, 0)),
                      pl.BlockSpec((cb, H, N), lambda i, s: (i, 0, 0))],
            out_specs=pl.BlockSpec((cb, J, N), lambda i, s: (i, 0, 0)),
            scratch_shapes=[pltpu.VMEM((cb, 2 * H, N), BF)]),
        out_shape=jax.ShapeDtypeStruct((C, J, N), BF),
        cost_estimate=pl.CostEstimate(flops=C * J * N * K * 2 * 3, bytes_accessed=2 * C * N * (2 * J + K), transcendentals=0),
        name="tri1",
    )(h, b, ao, ap)

def update_row(z, t, wg, wo, ng, nb, hg, hb):
    x = ln_cols(z, ng, nb).astype(BF)
    gate = jnp.dot(wg, x, preferred_element_type=F32)
    hid = ln_cols(t, hg, hb).astype(BF)
    o = jnp.dot(wo, hid, preferred_element_type=F32)
    return z + (0.5 * o) * (1.0 + jnp.tanh(0.5 * gate))

def fin0_body(s_ref, t_ref, z_ref, m_ref, wg, wo, ng, nb, hg, hb, wa, ng1, nb1, sel, mine_ref, theirs_ref, a_ref, ts, sa, ms):
    ch, n_cols = wo.shape[0], mine_ref.shape[1]
    ms[...] = 0.5 * m_ref[...].astype(F32)
    ts[...] = jnp.swapaxes(t_ref[...], 0, 1)
    def row(r, _):
        z1 = update_row(z_ref[r].astype(F32), ts[r].astype(F32), wg[...], wo[...], ng[...], nb[...], hg[...], hb[...]).astype(BF)
        cols = lax.dot_general(sel[...], z1, (((1,), (1,)), ((), ())), preferred_element_type=F32).astype(BF)
        mine_ref[r] = cols[:n_cols]
        theirs_ref[r] = cols[n_cols:]
        x = ln_cols(z1.astype(F32), ng1[...], nb1[...]).astype(BF)
        hm = ms[pl.ds(r, 1), :]
        q = jnp.dot(wa[...], x, preferred_element_type=F32)
        sa[r] = gated(q[:ch], q[ch:], hm).astype(BF)
        return 0
    lax.fori_loop(0, z_ref.shape[0], row, 0, unroll=2)
    a_ref[...] = jnp.swapaxes(sa[...], 0, 1)

def fin0(h, t, z, m, wts, rows=16):
    C, R, N = t.shape
    nblk = R // rows
    n_cols = wts[-1].shape[0] // 2
    full = lambda a: pl.BlockSpec(a.shape, lambda i, s: (0, 0))
    return pl.pallas_call(
        fin0_body,
        grid_spec=pltpu.PrefetchScalarGridSpec(
            num_scalar_prefetch=1, grid=(nblk,),
            in_specs=[pl.BlockSpec((C, rows, N), lambda i, s: (0, i, 0)),
                      pl.BlockSpec((rows, C, N), lambda i, s: (s[0] * nblk + i, 0, 0)),
                      pl.BlockSpec((rows, N), lambda i, s: (s[0] * nblk + i, 0))] + [full(w) for w in wts],
            out_specs=[pl.BlockSpec((rows, n_cols, C), lambda i, s: (i, 0, 0))] * 2
            + [pl.BlockSpec((C, rows, N), lambda i, s: (0, i, 0))],
            scratch_shapes=[pltpu.VMEM((rows, C, N), BF)] * 2 + [pltpu.VMEM((rows, N), F32)]),
        out_shape=[jax.ShapeDtypeStruct((R, n_cols, C), BF)] * 2 + [jax.ShapeDtypeStruct((C, R, N), BF)],
        cost_estimate=pl.CostEstimate(flops=R * N * C * C * 2 * 4 * 4, bytes_accessed=2 * C * N * R * 4, transcendentals=0),
        name="fin0",
    )(h, t, z, m, *wts)

def fin1_body(first, t_ref, z_ref, wg, wo, ng, nb, hg, hb, *rest):
    o_ref, ts, so = rest if first else rest[1:]
    ts[...] = jnp.swapaxes(t_ref[...], 0, 1)
    def row(r, _):
        z2 = update_row(z_ref[r].astype(F32), ts[r].astype(F32), wg[...], wo[...], ng[...], nb[...], hg[...], hb[...])
        so[r] = z2.T.astype(BF)
        return 0
    lax.fori_loop(0, z_ref.shape[0], row, 0, unroll=2)
    o_ref[...] = jnp.swapaxes(so[...], 0, 1)

def fin1(t, z, wts, crop, n_crops, buf, rows=16):
    C, J, N = t.shape
    full = lambda a: pl.BlockSpec(a.shape, lambda i: (0, 0))
    first = buf is None
    return pl.pallas_call(
        functools.partial(fin1_body, first),
        grid=(J // rows,),
        in_specs=[pl.BlockSpec((C, rows, N), lambda i: (0, i, 0)),
                  pl.BlockSpec((rows, C, N), lambda i: (i, 0, 0))] + [full(w) for w in wts]
        + ([] if first else [pl.BlockSpec(memory_space=pl.ANY)]),
        out_specs=pl.BlockSpec((None, N, rows, C), lambda i: (crop, 0, i, 0)),
        scratch_shapes=[pltpu.VMEM((rows, C, N), BF), pltpu.VMEM((rows, N, C), BF)],
        out_shape=jax.ShapeDtypeStruct((n_crops, N, J, C), BF),
        input_output_aliases={} if first else {2 + len(wts): 0},
        cost_estimate=pl.CostEstimate(flops=J * N * C * C * 2 * 2 * 4, bytes_accessed=2 * C * N * J * 3, transcendentals=0),
        name="fin1",
    )(t, z, *wts, *([] if first else [buf]))


def solution(mesh):
    n_dev = mesh.shape['dap']
    swap = [(i, i ^ 1) for i in range(n_dev)]

    def shard_body(pair_stack, mask_stack, norm_gain, norm_bias, w_proj, w_gate, hid_gain, hid_bias, w_out):
        n_crops, rows, n_res, ch = pair_stack.shape
        half = n_res // 2
        dev = lax.axis_index('dap')
        side = dev % 2
        side_arr = jnp.reshape(side, (1,)).astype(jnp.int32)
        zero_arr = jnp.zeros((1,), jnp.int32)
        col = lambda v: v.astype(F32).reshape(-1, 1)
        wts = [(w_gate[u].T, w_out[u].T, col(norm_gain[u]), col(norm_bias[u]), col(hid_gain[u]), col(hid_bias[u]))
               for u in range(2)]
        wp = [w_proj[u].T for u in range(2)]
        ln1 = (wts[1][2], wts[1][3])

        mask_all = lax.all_gather(mask_stack.astype(BF), 'dap', axis=1, tiled=True)
        mask_cols = jnp.swapaxes(lax.dynamic_slice_in_dim(mask_all, dev * rows, rows, 2), 1, 2)

        pick = jnp.concatenate([dev * rows + jnp.arange(rows), (dev ^ 1) * rows + jnp.arange(rows)])
        sel = (pick[:, None] == jnp.arange(n_res)[None, :]).astype(BF)
        blocks = [jnp.swapaxes(pair_stack[crop], 1, 2) for crop in range(n_crops)]
        out = prev = None
        for crop in range(n_crops + 1):
            if crop < n_crops:
                z_all = lax.all_gather(blocks[crop], 'dap', axis=0, tiled=True)
                mask = mask_all[crop]
                a0, b0 = proj(z_all, mask, side_arr, half // 16, wp[0], wts[0][2], wts[0][3], 2)
                b0p = lax.ppermute(b0, 'dap', swap)
            if prev is not None:
                a1, a1p, z1_cols = prev
                if crop < n_crops:
                    a0, a1, a1p, z1_cols = lax.optimization_barrier((a0, a1, a1p, z1_cols))
                b1, = proj(z1_cols, mask_cols[crop - 1], zero_arr, rows // 16, wp[1][2 * ch:], *ln1, 1)
                t1 = tri1(side_arr, b1, a1, a1p)
                if crop < n_crops:
                    a0, t1 = lax.optimization_barrier((a0, t1))
                out = fin1(t1, z1_cols, wts[1], crop - 1, n_crops, out)
            if crop < n_crops:
                t0 = tri0(side_arr, a0, b0, b0p)
                mine, theirs, a1 = fin0(side_arr, t0, z_all, mask, wts[0] + (wp[1][:2 * ch],) + ln1 + (sel,))
                if crop + AHEAD < n_crops:
                    mine, blocks[crop + AHEAD] = lax.optimization_barrier((mine, blocks[crop + AHEAD]))
                a1p = lax.ppermute(a1, 'dap', swap)
                theirs = lax.ppermute(theirs, 'dap', swap)
                lo = jnp.where(side == 0, mine, theirs)
                hi = jnp.where(side == 0, theirs, mine)
                prev = a1, a1p, jnp.transpose(jnp.concatenate([lo, hi], 0), (1, 2, 0))
        return out

    rep = P()
    in_specs = (P('data', 'dap', None, None), P('data', 'dap', None)) + (rep,) * 7
    return jax.shard_map(shard_body, mesh=mesh, in_specs=in_specs,
                         out_specs=P('data', None, 'dap', None), check_vma=False)
```

```python
import functools, jax, jax.numpy as jnp
from jax import lax
from jax.experimental import pallas as pl
from jax.experimental.pallas import tpu as pltpu
from jax.sharding import PartitionSpec as P


EPS = 1e-5
UNROLL = 8
CB = 16
BF = jnp.bfloat16
F32 = jnp.float32

def ln_cols(v, g, b):
    mu = jnp.mean(v, axis=0, keepdims=True)
    cen = v - mu
    var = jnp.mean(cen * cen, axis=0, keepdims=True)
    return cen * lax.rsqrt(var + EPS) * g + b

def gated(p, g, mask):
    return (p * mask) * (1.0 + jnp.tanh(g))


def turn_body(z_ref, o_ref):
    def row(r, _):
        o_ref[r] = z_ref[r].T
        return 0

    lax.fori_loop(0, z_ref.shape[0], row, 0, unroll=4)


def turn(z, crop, rows=16):
    _, R, N, C = z.shape
    return pl.pallas_call(
        turn_body,
        grid=(R // rows,),
        in_specs=[pl.BlockSpec((None, rows, N, C), lambda i: (crop, i, 0, 0))],
        out_specs=pl.BlockSpec((rows, C, N), lambda i: (i, 0, 0)),
        out_shape=jax.ShapeDtypeStruct((R, C, N), BF),
        cost_estimate=pl.CostEstimate(flops=R * N * C * 60, bytes_accessed=4 * R * N * C, transcendentals=0),
        name="turn",
    )(z)


def proj0_body(s_ref, z_ref, m_ref, w_ref, g_ref, b_ref, x_ref, a_ref, b_out_ref, sa, sb, ms):
    ch = g_ref.shape[0]
    ms[...] = m_ref[...].astype(F32)

    def row(r, _):
        x = ln_cols(z_ref[r].astype(F32), g_ref[...], b_ref[...]).astype(BF)
        x_ref[r] = x
        q = jnp.dot(w_ref[...], x, preferred_element_type=F32)
        mask = ms[pl.ds(r, 1), :]
        sa[r] = gated(q[:ch], q[ch:2 * ch], mask).astype(BF)
        sb[r] = gated(q[2 * ch:3 * ch], q[3 * ch:], mask).astype(BF)
        return 0

    lax.fori_loop(0, z_ref.shape[0], row, 0, unroll=UNROLL)
    a_ref[...] = jnp.swapaxes(sa[...], 0, 1)
    b_out_ref[...] = jnp.swapaxes(sb[...], 0, 1)


def proj0(side, z, m, w_t, g, b, rows=16):
    R, C, N = z.shape
    nblk = R // 2 // rows
    full = lambda a: pl.BlockSpec(a.shape, lambda i, s: (0, 0))
    return pl.pallas_call(
        proj0_body,
        grid_spec=pltpu.PrefetchScalarGridSpec(
            num_scalar_prefetch=1, grid=(nblk,),
            in_specs=[pl.BlockSpec((rows, C, N), lambda i, s: (s[0] * nblk + i, 0, 0)),
                      pl.BlockSpec((rows, N), lambda i, s: (s[0] * nblk + i, 0)), full(w_t), full(g), full(b)],
            out_specs=[pl.BlockSpec((rows, C, N), lambda i, s: (i, 0, 0))]
            + [pl.BlockSpec((C, rows, N), lambda i, s: (0, i, 0))] * 2,
            scratch_shapes=[pltpu.VMEM((rows, C, N), BF)] * 2 + [pltpu.VMEM((rows, N), F32)]),
        out_shape=[jax.ShapeDtypeStruct((R // 2, C, N), BF)] + [jax.ShapeDtypeStruct((C, R // 2, N), BF)] * 2,
        cost_estimate=pl.CostEstimate(flops=R * N * C * C * 16, bytes_accessed=4 * R * N * C, transcendentals=0),
        name="proj0",
    )(side, z, m, w_t, g, b)


def proj1_body(s_ref, mine_ref, theirs_ref, m_ref, w_ref, g_ref, b_ref, z_ref, x_ref, b_out_ref, zz, sb, ms):
    ch = g_ref.shape[0]
    half = mine_ref.shape[1]
    side = s_ref[0]
    ms[...] = m_ref[...].astype(F32)
    zz[:, pl.ds(pl.multiple_of(side * half, 16), half), :] = mine_ref[...]
    zz[:, pl.ds(pl.multiple_of((1 - side) * half, 16), half), :] = theirs_ref[...]

    def col(r, _):
        z = zz[r].T
        z_ref[r] = z
        x = ln_cols(z.astype(F32), g_ref[...], b_ref[...]).astype(BF)
        x_ref[r] = x
        q = jnp.dot(w_ref[...], x, preferred_element_type=F32)
        sb[r] = gated(q[:ch], q[ch:], ms[pl.ds(r, 1), :]).astype(BF)
        return 0

    lax.fori_loop(0, zz.shape[0], col, 0, unroll=4)
    b_out_ref[...] = jnp.swapaxes(sb[...], 0, 1)


def proj1(side, mine, other, m, w_t, g, b):
    cols, H, N = mine.shape
    C = g.shape[0]
    J = cols * (N // C)
    full = lambda a: pl.BlockSpec(a.shape, lambda i, s: (0, 0))
    wide = lambda: pl.BlockSpec((cols, C, N), lambda i, s: (i, 0, 0))
    return pl.pallas_call(
        proj1_body,
        grid_spec=pltpu.PrefetchScalarGridSpec(
            num_scalar_prefetch=1, grid=(J // cols,),
            in_specs=[pl.BlockSpec((cols, H, C), lambda i, s: (0, 0, i)),
                      pl.BlockSpec((cols, H, C), lambda i, s: (C // cols, 0, i))]
            + [pl.BlockSpec((cols, N), lambda i, s: (i, 0)), full(w_t), full(g), full(b)],
            out_specs=[wide(), wide(), pl.BlockSpec((C, cols, N), lambda i, s: (0, i, 0))],
            scratch_shapes=[pltpu.VMEM((cols, N, C), BF), pltpu.VMEM((cols, C, N), BF), pltpu.VMEM((cols, N), F32)]),
        out_shape=[jax.ShapeDtypeStruct((J, C, N), BF)] * 2 + [jax.ShapeDtypeStruct((C, J, N), BF)],
        cost_estimate=pl.CostEstimate(flops=J * N * C * C * 16, bytes_accessed=8 * J * N * C, transcendentals=0),
        name="proj1",
    )(side, mine, other, m, w_t, g, b)


def tri0_body(s_ref, a_ref, bo_ref, bp_ref, t_ref, bs):
    half = bo_ref.shape[1]
    h = s_ref[0]
    o0 = pl.multiple_of(h * half, 16)
    o1 = pl.multiple_of((1 - h) * half, 16)
    bs[:, pl.ds(o0, half), :] = bo_ref[...]
    bs[:, pl.ds(o1, half), :] = bp_ref[...]
    def one(c, _):
        t_ref[c] = lax.dot_general(a_ref[c], bs[c], (((1,), (1,)), ((), ())), preferred_element_type=F32).astype(BF)
        return 0
    lax.fori_loop(0, a_ref.shape[0], one, 0, unroll=4)

def tri0(h, a, bo, bp, cb=CB):
    C, R, N = a.shape
    H = bo.shape[1]
    return pl.pallas_call(
        tri0_body,
        grid_spec=pltpu.PrefetchScalarGridSpec(
            num_scalar_prefetch=1, grid=(C // cb,),
            in_specs=[pl.BlockSpec((cb, R, N), lambda i, s: (i, 0, 0)),
                      pl.BlockSpec((cb, H, N), lambda i, s: (i, 0, 0)),
                      pl.BlockSpec((cb, H, N), lambda i, s: (i, 0, 0))],
            out_specs=pl.BlockSpec((cb, R, 2 * H), lambda i, s: (i, 0, 0)),
            scratch_shapes=[pltpu.VMEM((cb, 2 * H, N), BF)]),
        out_shape=jax.ShapeDtypeStruct((C, R, 2 * H), BF),
        cost_estimate=pl.CostEstimate(flops=C * R * N * 2 * H * 2, bytes_accessed=2 * C * N * (2 * R + 2 * H), transcendentals=0),
        name="tri0",
    )(h, a, bo, bp)

def tri1_body(s_ref, b_ref, ao_ref, ap_ref, t_ref, asc):
    half = ao_ref.shape[1]
    h = s_ref[0]
    o0 = pl.multiple_of(h * half, 16)
    o1 = pl.multiple_of((1 - h) * half, 16)
    asc[:, pl.ds(o0, half), :] = ao_ref[...]
    asc[:, pl.ds(o1, half), :] = ap_ref[...]
    def one(c, _):
        t_ref[c] = jnp.dot(b_ref[c], asc[c], preferred_element_type=F32).astype(BF)
        return 0
    lax.fori_loop(0, b_ref.shape[0], one, 0, unroll=4)

def tri1(h, b, ao, ap, cb=CB):
    C, J, K = b.shape
    H, N = ao.shape[1:]
    return pl.pallas_call(
        tri1_body,
        grid_spec=pltpu.PrefetchScalarGridSpec(
            num_scalar_prefetch=1, grid=(C // cb,),
            in_specs=[pl.BlockSpec((cb, J, K), lambda i, s: (i, 0, 0)),
                      pl.BlockSpec((cb, H, N), lambda i, s: (i, 0, 0)),
                      pl.BlockSpec((cb, H, N), lambda i, s: (i, 0, 0))],
            out_specs=pl.BlockSpec((cb, J, N), lambda i, s: (i, 0, 0)),
            scratch_shapes=[pltpu.VMEM((cb, 2 * H, N), BF)]),
        out_shape=jax.ShapeDtypeStruct((C, J, N), BF),
        cost_estimate=pl.CostEstimate(flops=C * J * N * K * 2 * 3, bytes_accessed=2 * C * N * (2 * J + K), transcendentals=0),
        name="tri1",
    )(h, b, ao, ap)

def update_cols(z, x, t, wg, wo, hg, hb):
    gate = jnp.dot(wg, x, preferred_element_type=F32)
    hid = ln_cols(t.astype(F32), hg, hb).astype(BF)
    o = jnp.dot(wo, hid, preferred_element_type=F32)
    return z.astype(F32) + o * (1.0 + jnp.tanh(gate))


def fin0_body(s_ref, t_ref, z_ref, x_ref, m_ref, wg, wo, hg, hb, wa, ng, nb, sel, mine_ref, a_ref, ts, sa, sm, ms):
    ch, per = wo.shape[0], mine_ref.shape[0]
    n_cols = sel.shape[0] // 2
    ms[...] = m_ref[...].astype(F32)
    ts[...] = jnp.swapaxes(t_ref[...], 0, 1)

    def row(r, _):
        z1 = update_cols(z_ref[r], x_ref[r], ts[r], wg[...], wo[...], hg[...], hb[...]).astype(BF)
        cols = lax.dot_general(sel[...], z1, (((1,), (1,)), ((), ())), preferred_element_type=F32).astype(BF)
        sm[r] = jnp.concatenate([cols[k:k + per] for k in range(0, n_cols, per)], axis=1)
        sa[r, ch:] = jnp.concatenate([cols[k:k + per] for k in range(n_cols, 2 * n_cols, per)], axis=1)
        x1 = ln_cols(z1.astype(F32), ng[...], nb[...]).astype(BF)
        q = jnp.dot(wa[...], x1, preferred_element_type=F32)
        sa[r, :ch] = gated(q[:ch], q[ch:], ms[pl.ds(r, 1), :]).astype(BF)
        return 0

    lax.fori_loop(0, z_ref.shape[0], row, 0, unroll=UNROLL)
    a_ref[...] = jnp.swapaxes(sa[...], 0, 1)
    mine_ref[...] = jnp.swapaxes(sm[...], 0, 1)


def fin0(side, t, z, x, m, wts, rows=16):
    C, R, N = t.shape
    nblk = R // rows
    per = wts[-1].shape[0] // 2 * C // N
    full = lambda a: pl.BlockSpec(a.shape, lambda i, s: (0, 0))
    return pl.pallas_call(
        fin0_body,
        grid_spec=pltpu.PrefetchScalarGridSpec(
            num_scalar_prefetch=1, grid=(nblk,),
            in_specs=[pl.BlockSpec((C, rows, N), lambda i, s: (0, i, 0)),
                      pl.BlockSpec((rows, C, N), lambda i, s: (s[0] * nblk + i, 0, 0)),
                      pl.BlockSpec((rows, C, N), lambda i, s: (i, 0, 0)),
                      pl.BlockSpec((rows, N), lambda i, s: (s[0] * nblk + i, 0))] + [full(w) for w in wts],
            out_specs=[pl.BlockSpec((n, rows, N), lambda i, s: (0, i, 0)) for n in (per, C + per)],
            scratch_shapes=[pltpu.VMEM((rows, n, N), BF) for n in (C, C + per, per)] + [pltpu.VMEM((rows, N), F32)]),
        out_shape=[jax.ShapeDtypeStruct((n, R, N), BF) for n in (per, C + per)],
        cost_estimate=pl.CostEstimate(flops=R * N * C * C * 32, bytes_accessed=8 * C * N * R, transcendentals=0),
        name="fin0",
    )(side, t, z, x, m, *wts)


def fin1_body(first, t_ref, z_ref, x_ref, wg, wo, hg, hb, *rest):
    o_ref, ts, so = rest if first else rest[1:]
    ts[...] = jnp.swapaxes(t_ref[...], 0, 1)

    def row(r, _):
        z2 = update_cols(z_ref[r], x_ref[r], ts[r], wg[...], wo[...], hg[...], hb[...])
        so[r] = z2.T.astype(BF)
        return 0

    lax.fori_loop(0, z_ref.shape[0], row, 0, unroll=4)
    o_ref[...] = jnp.swapaxes(so[...], 0, 1)


def fin1(t, z, x, wts, crop, n_crops, buf, rows=16):
    C, J, N = t.shape
    full = lambda a: pl.BlockSpec(a.shape, lambda i: (0, 0))
    first = buf is None
    return pl.pallas_call(
        functools.partial(fin1_body, first),
        grid=(J // rows,),
        in_specs=[pl.BlockSpec((C, rows, N), lambda i: (0, i, 0)),
                  pl.BlockSpec((rows, C, N), lambda i: (i, 0, 0)),
                  pl.BlockSpec((rows, C, N), lambda i: (i, 0, 0))] + [full(w) for w in wts]
        + ([] if first else [pl.BlockSpec(memory_space=pl.ANY)]),
        out_specs=pl.BlockSpec((None, N, rows, C), lambda i: (crop, 0, i, 0)),
        scratch_shapes=[pltpu.VMEM((rows, C, N), BF), pltpu.VMEM((rows, N, C), BF)],
        out_shape=jax.ShapeDtypeStruct((n_crops, N, J, C), BF),
        input_output_aliases={} if first else {3 + len(wts): 0},
        cost_estimate=pl.CostEstimate(flops=J * N * C * C * 16, bytes_accessed=8 * C * N * J, transcendentals=0),
        name="fin1",
    )(t, z, x, *wts, *([] if first else [buf]))


def solution(mesh):
    n_dev = mesh.shape['dap']
    swap = [(i, i ^ 1) for i in range(n_dev)]

    def shard_body(pair_stack, mask_stack, norm_gain, norm_bias, w_proj, w_gate, hid_gain, hid_bias, w_out):
        n_crops, rows, n_res, ch = pair_stack.shape
        dev = lax.axis_index('dap')
        side = jnp.reshape(dev % 2, (1,)).astype(jnp.int32)
        col = lambda v: v.astype(F32).reshape(-1, 1)
        fin = [(0.5 * w_gate[u].T, 0.5 * w_out[u].T, col(hid_gain[u]), col(hid_bias[u])) for u in range(2)]
        wp = [0.5 * w_proj[u].T for u in range(2)]
        ln = [(col(norm_gain[u]), col(norm_bias[u])) for u in range(2)]
        pick = jnp.concatenate([dev * rows + jnp.arange(rows), (dev ^ 1) * rows + jnp.arange(rows)])
        sel = (pick[:, None] == jnp.arange(n_res)[None, :]).astype(BF)

        mask_all = lax.all_gather(mask_stack.astype(BF), 'dap', axis=1, tiled=True)
        mask_cols = jnp.swapaxes(lax.dynamic_slice_in_dim(mask_all, dev * rows, rows, 2), 1, 2)
        z_all = [lax.all_gather(turn(pair_stack, crop), 'dap', axis=0, tiled=True) for crop in range(n_crops)]

        projs, halves, sums = {}, {}, {}
        last = [None]

        def after_last(args):
            if last[0] is None:
                return args
            table, key = last[0]
            head, *tail = table[key]
            head, *args = lax.optimization_barrier((head, *args))
            table[key] = (head, *tail)
            return args

        def project(crop):
            z_all[crop], = after_last([z_all[crop]])
            x0, a0, b0 = proj0(side, z_all[crop], mask_all[crop], wp[0], *ln[0])
            projs[crop] = a0, b0, lax.ppermute(b0, 'dap', swap), x0
            last[0] = projs, crop

        def outgoing(crop):
            a0, b0, b0p, x0 = projs[crop]
            b0, b0p = after_last([b0, b0p])
            a0 = projs[crop][0]
            t0 = tri0(side, a0, b0, b0p)
            mine, a1 = fin0(side, t0, z_all[crop], x0, mask_all[crop], fin[0] + (wp[1][:2 * ch],) + ln[1] + (sel,))
            halves[crop] = mine, a1, lax.ppermute(a1, 'dap', swap)
            last[0] = halves, crop

        def incoming(crop):
            mine, a1, a1p = halves[crop]
            a1, a1p = after_last([a1, a1p])
            mine = halves[crop][0]
            z1, x1, b1 = proj1(side, mine, a1p, mask_cols[crop], wp[1][2 * ch:], *ln[1])
            sums[crop] = tri1(side, b1, a1, a1p), z1, x1
            last[0] = sums, crop

        steps = []
        for crop in range(n_crops):
            if crop < 3:
                steps += [(project, crop)] + ([(incoming, crop - 1)] if crop == 1 else []) + ([(outgoing, crop)] if crop < 2 else [])
            else:
                steps += [(project, crop), (outgoing, crop - 1), (incoming, crop - 2)]
        done = set(steps)
        steps += [(f, c) for c in range(n_crops) for f in (outgoing, incoming) if (f, c) not in done]
        out = None
        for f, crop in steps:
            waiting = list(sums)
            f(crop)
            for c in waiting:
                t1, z1, x1 = sums.pop(c)
                out = fin1(t1, z1, x1, fin[1], c, n_crops, out)
        for c in list(sums):
            t1, z1, x1 = sums.pop(c)
            out = fin1(t1, z1, x1, fin[1], c, n_crops, out)
        return out

    rep = P()
    in_specs = (P('data', 'dap', None, None), P('data', 'dap', None)) + (rep,) * 7
    return jax.shard_map(shard_body, mesh=mesh, in_specs=in_specs,
                         out_specs=P('data', None, 'dap', None), check_vma=False)
```

```python
import functools, jax, jax.numpy as jnp
from jax import lax
from jax.experimental import pallas as pl
from jax.experimental.pallas import tpu as pltpu
from jax.sharding import PartitionSpec as P


EPS = 1e-5
UNROLL = 16
LEAD = 4
CB = 16
BF = jnp.bfloat16
F32 = jnp.float32

def ln_cols(v, g, b):
    mu = jnp.mean(v, axis=0, keepdims=True)
    cen = v - mu
    var = jnp.mean(cen * cen, axis=0, keepdims=True)
    return cen * lax.rsqrt(var + EPS) * g + b

def gated(p, g, mask):
    return (p * mask) * (1.0 + jnp.tanh(g))


def turn_body(z_ref, o_ref):
    def row(r, _):
        o_ref[r] = z_ref[r].T
        return 0

    lax.fori_loop(0, z_ref.shape[0], row, 0, unroll=4)


def turn(z, crop, rows=16):
    _, R, N, C = z.shape
    return pl.pallas_call(
        turn_body,
        grid=(R // rows,),
        in_specs=[pl.BlockSpec((None, rows, N, C), lambda i: (crop, i, 0, 0))],
        out_specs=pl.BlockSpec((rows, C, N), lambda i: (i, 0, 0)),
        out_shape=jax.ShapeDtypeStruct((R, C, N), BF),
        cost_estimate=pl.CostEstimate(flops=R * N * C * 60, bytes_accessed=4 * R * N * C, transcendentals=0),
        name="turn",
    )(z)


def proj0_body(s_ref, z_ref, m_ref, w_ref, g_ref, b_ref, x_ref, a_ref, b_out_ref, sa, sb, ms):
    ch = g_ref.shape[0]
    ms[...] = m_ref[...].astype(F32)

    def row(r, _):
        x = ln_cols(z_ref[r].astype(F32), g_ref[...], b_ref[...]).astype(BF)
        x_ref[r] = x
        q = jnp.dot(w_ref[...], x, preferred_element_type=F32)
        mask = ms[pl.ds(r, 1), :]
        sa[r] = gated(q[:ch], q[ch:2 * ch], mask).astype(BF)
        sb[r] = gated(q[2 * ch:3 * ch], q[3 * ch:], mask).astype(BF)
        return 0

    lax.fori_loop(0, z_ref.shape[0], row, 0, unroll=UNROLL)
    a_ref[...] = jnp.swapaxes(sa[...], 0, 1)
    b_out_ref[...] = jnp.swapaxes(sb[...], 0, 1)


def proj0(side, z, m, w_t, g, b, rows=16):
    R, C, N = z.shape
    nblk = R // 2 // rows
    full = lambda a: pl.BlockSpec(a.shape, lambda i, s: (0, 0))
    return pl.pallas_call(
        proj0_body,
        grid_spec=pltpu.PrefetchScalarGridSpec(
            num_scalar_prefetch=1, grid=(nblk,),
            in_specs=[pl.BlockSpec((rows, C, N), lambda i, s: (s[0] * nblk + i, 0, 0)),
                      pl.BlockSpec((rows, N), lambda i, s: (s[0] * nblk + i, 0)), full(w_t), full(g), full(b)],
            out_specs=[pl.BlockSpec((rows, C, N), lambda i, s: (i, 0, 0))]
            + [pl.BlockSpec((C, rows, N), lambda i, s: (0, i, 0))] * 2,
            scratch_shapes=[pltpu.VMEM((rows, C, N), BF)] * 2 + [pltpu.VMEM((rows, N), F32)]),
        out_shape=[jax.ShapeDtypeStruct((R // 2, C, N), BF)] + [jax.ShapeDtypeStruct((C, R // 2, N), BF)] * 2,
        cost_estimate=pl.CostEstimate(flops=R * N * C * C * 16, bytes_accessed=4 * R * N * C, transcendentals=0),
        name="proj0",
    )(side, z, m, w_t, g, b)


def proj1_body(s_ref, mine_ref, theirs_ref, m_ref, w_ref, g_ref, b_ref, z_ref, x_ref, b_out_ref, zz, sb, ms):
    ch = g_ref.shape[0]
    half = mine_ref.shape[1]
    side = s_ref[0]
    ms[...] = m_ref[...].astype(F32)
    zz[:, pl.ds(pl.multiple_of(side * half, 16), half), :] = mine_ref[...]
    zz[:, pl.ds(pl.multiple_of((1 - side) * half, 16), half), :] = theirs_ref[...]

    def col(r, _):
        z = zz[r].T
        z_ref[r] = z
        x = ln_cols(z.astype(F32), g_ref[...], b_ref[...]).astype(BF)
        x_ref[r] = x
        q = jnp.dot(w_ref[...], x, preferred_element_type=F32)
        sb[r] = gated(q[:ch], q[ch:], ms[pl.ds(r, 1), :]).astype(BF)
        return 0

    lax.fori_loop(0, zz.shape[0], col, 0, unroll=4)
    b_out_ref[...] = jnp.swapaxes(sb[...], 0, 1)


def proj1(side, mine, other, m, w_t, g, b):
    cols, H, N = mine.shape
    C = g.shape[0]
    J = cols * (N // C)
    full = lambda a: pl.BlockSpec(a.shape, lambda i, s: (0, 0))
    wide = lambda: pl.BlockSpec((cols, C, N), lambda i, s: (i, 0, 0))
    return pl.pallas_call(
        proj1_body,
        grid_spec=pltpu.PrefetchScalarGridSpec(
            num_scalar_prefetch=1, grid=(J // cols,),
            in_specs=[pl.BlockSpec((cols, H, C), lambda i, s: (0, 0, i)),
                      pl.BlockSpec((cols, H, C), lambda i, s: (C // cols, 0, i))]
            + [pl.BlockSpec((cols, N), lambda i, s: (i, 0)), full(w_t), full(g), full(b)],
            out_specs=[wide(), wide(), pl.BlockSpec((C, cols, N), lambda i, s: (0, i, 0))],
            scratch_shapes=[pltpu.VMEM((cols, N, C), BF), pltpu.VMEM((cols, C, N), BF), pltpu.VMEM((cols, N), F32)]),
        out_shape=[jax.ShapeDtypeStruct((J, C, N), BF)] * 2 + [jax.ShapeDtypeStruct((C, J, N), BF)],
        cost_estimate=pl.CostEstimate(flops=J * N * C * C * 16, bytes_accessed=8 * J * N * C, transcendentals=0),
        name="proj1",
    )(side, mine, other, m, w_t, g, b)


def tri0_body(s_ref, a_ref, bo_ref, bp_ref, t_ref, bs):
    half = bo_ref.shape[1]
    h = s_ref[0]
    o0 = pl.multiple_of(h * half, 16)
    o1 = pl.multiple_of((1 - h) * half, 16)
    bs[:, pl.ds(o0, half), :] = bo_ref[...]
    bs[:, pl.ds(o1, half), :] = bp_ref[...]
    def one(c, _):
        t_ref[c] = lax.dot_general(a_ref[c], bs[c], (((1,), (1,)), ((), ())), preferred_element_type=F32).astype(BF)
        return 0
    lax.fori_loop(0, a_ref.shape[0], one, 0, unroll=4)

def tri0(h, a, bo, bp, cb=CB):
    C, R, N = a.shape
    H = bo.shape[1]
    return pl.pallas_call(
        tri0_body,
        grid_spec=pltpu.PrefetchScalarGridSpec(
            num_scalar_prefetch=1, grid=(C // cb,),
            in_specs=[pl.BlockSpec((cb, R, N), lambda i, s: (i, 0, 0)),
                      pl.BlockSpec((cb, H, N), lambda i, s: (i, 0, 0)),
                      pl.BlockSpec((cb, H, N), lambda i, s: (i, 0, 0))],
            out_specs=pl.BlockSpec((cb, R, 2 * H), lambda i, s: (i, 0, 0)),
            scratch_shapes=[pltpu.VMEM((cb, 2 * H, N), BF)]),
        out_shape=jax.ShapeDtypeStruct((C, R, 2 * H), BF),
        cost_estimate=pl.CostEstimate(flops=C * R * N * 2 * H * 2, bytes_accessed=2 * C * N * (2 * R + 2 * H), transcendentals=0),
        name="tri0",
    )(h, a, bo, bp)

def tri1_body(s_ref, b_ref, ao_ref, ap_ref, t_ref, asc):
    half = ao_ref.shape[1]
    h = s_ref[0]
    o0 = pl.multiple_of(h * half, 16)
    o1 = pl.multiple_of((1 - h) * half, 16)
    asc[:, pl.ds(o0, half), :] = ao_ref[...]
    asc[:, pl.ds(o1, half), :] = ap_ref[...]
    def one(c, _):
        t_ref[c] = jnp.dot(b_ref[c], asc[c], preferred_element_type=F32).astype(BF)
        return 0
    lax.fori_loop(0, b_ref.shape[0], one, 0, unroll=4)

def tri1(h, b, ao, ap, cb=CB):
    C, J, K = b.shape
    H, N = ao.shape[1:]
    return pl.pallas_call(
        tri1_body,
        grid_spec=pltpu.PrefetchScalarGridSpec(
            num_scalar_prefetch=1, grid=(C // cb,),
            in_specs=[pl.BlockSpec((cb, J, K), lambda i, s: (i, 0, 0)),
                      pl.BlockSpec((cb, H, N), lambda i, s: (i, 0, 0)),
                      pl.BlockSpec((cb, H, N), lambda i, s: (i, 0, 0))],
            out_specs=pl.BlockSpec((cb, J, N), lambda i, s: (i, 0, 0)),
            scratch_shapes=[pltpu.VMEM((cb, 2 * H, N), BF)]),
        out_shape=jax.ShapeDtypeStruct((C, J, N), BF),
        cost_estimate=pl.CostEstimate(flops=C * J * N * K * 2 * 3, bytes_accessed=2 * C * N * (2 * J + K), transcendentals=0),
        name="tri1",
    )(h, b, ao, ap)

def update_cols(z, x, t, wg, wo, hg, hb):
    gate = jnp.dot(wg, x, preferred_element_type=F32)
    hid = ln_cols(t.astype(F32), hg, hb).astype(BF)
    o = jnp.dot(wo, hid, preferred_element_type=F32)
    return z.astype(F32) + o * (1.0 + jnp.tanh(gate))


def fin0_body(s_ref, t_ref, z_ref, x_ref, m_ref, wg, wo, hg, hb, wa, ng, nb, sel, mine_ref, a_ref, ts, sa, sm, ms):
    ch, per = wo.shape[0], mine_ref.shape[0]
    n_cols = sel.shape[0] // 2
    ms[...] = m_ref[...].astype(F32)
    ts[...] = jnp.swapaxes(t_ref[...], 0, 1)

    def row(r, _):
        z1 = update_cols(z_ref[r], x_ref[r], ts[r], wg[...], wo[...], hg[...], hb[...]).astype(BF)
        cols = lax.dot_general(sel[...], z1, (((1,), (1,)), ((), ())), preferred_element_type=F32).astype(BF)
        sm[r] = jnp.concatenate([cols[k:k + per] for k in range(0, n_cols, per)], axis=1)
        sa[r, ch:] = jnp.concatenate([cols[k:k + per] for k in range(n_cols, 2 * n_cols, per)], axis=1)
        x1 = ln_cols(z1.astype(F32), ng[...], nb[...]).astype(BF)
        q = jnp.dot(wa[...], x1, preferred_element_type=F32)
        sa[r, :ch] = gated(q[:ch], q[ch:], ms[pl.ds(r, 1), :]).astype(BF)
        return 0

    lax.fori_loop(0, z_ref.shape[0], row, 0, unroll=UNROLL)
    a_ref[...] = jnp.swapaxes(sa[...], 0, 1)
    mine_ref[...] = jnp.swapaxes(sm[...], 0, 1)


def fin0(side, t, z, x, m, wts, rows=16):
    C, R, N = t.shape
    nblk = R // rows
    per = wts[-1].shape[0] // 2 * C // N
    full = lambda a: pl.BlockSpec(a.shape, lambda i, s: (0, 0))
    return pl.pallas_call(
        fin0_body,
        grid_spec=pltpu.PrefetchScalarGridSpec(
            num_scalar_prefetch=1, grid=(nblk,),
            in_specs=[pl.BlockSpec((C, rows, N), lambda i, s: (0, i, 0)),
                      pl.BlockSpec((rows, C, N), lambda i, s: (s[0] * nblk + i, 0, 0)),
                      pl.BlockSpec((rows, C, N), lambda i, s: (i, 0, 0)),
                      pl.BlockSpec((rows, N), lambda i, s: (s[0] * nblk + i, 0))] + [full(w) for w in wts],
            out_specs=[pl.BlockSpec((n, rows, N), lambda i, s: (0, i, 0)) for n in (per, C + per)],
            scratch_shapes=[pltpu.VMEM((rows, n, N), BF) for n in (C, C + per, per)] + [pltpu.VMEM((rows, N), F32)]),
        out_shape=[jax.ShapeDtypeStruct((n, R, N), BF) for n in (per, C + per)],
        cost_estimate=pl.CostEstimate(flops=R * N * C * C * 32, bytes_accessed=8 * C * N * R, transcendentals=0),
        name="fin0",
    )(side, t, z, x, m, *wts)


def fin1_body(first, t_ref, z_ref, x_ref, wg, wo, hg, hb, *rest):
    o_ref, ts, so = rest if first else rest[1:]
    ts[...] = jnp.swapaxes(t_ref[...], 0, 1)

    def row(r, _):
        z2 = update_cols(z_ref[r], x_ref[r], ts[r], wg[...], wo[...], hg[...], hb[...])
        so[r] = z2.T.astype(BF)
        return 0

    lax.fori_loop(0, z_ref.shape[0], row, 0, unroll=4)
    o_ref[...] = jnp.swapaxes(so[...], 0, 1)


def fin1(t, z, x, wts, crop, n_crops, buf, rows=16):
    C, J, N = t.shape
    full = lambda a: pl.BlockSpec(a.shape, lambda i: (0, 0))
    first = buf is None
    return pl.pallas_call(
        functools.partial(fin1_body, first),
        grid=(J // rows,),
        in_specs=[pl.BlockSpec((C, rows, N), lambda i: (0, i, 0)),
                  pl.BlockSpec((rows, C, N), lambda i: (i, 0, 0)),
                  pl.BlockSpec((rows, C, N), lambda i: (i, 0, 0))] + [full(w) for w in wts]
        + ([] if first else [pl.BlockSpec(memory_space=pl.ANY)]),
        out_specs=pl.BlockSpec((None, N, rows, C), lambda i: (crop, 0, i, 0)),
        scratch_shapes=[pltpu.VMEM((rows, C, N), BF), pltpu.VMEM((rows, N, C), BF)],
        out_shape=jax.ShapeDtypeStruct((n_crops, N, J, C), BF),
        input_output_aliases={} if first else {3 + len(wts): 0},
        cost_estimate=pl.CostEstimate(flops=J * N * C * C * 16, bytes_accessed=8 * C * N * J, transcendentals=0),
        name="fin1",
    )(t, z, x, *wts, *([] if first else [buf]))


def solution(mesh):
    n_dev = mesh.shape['dap']
    swap = [(i, i ^ 1) for i in range(n_dev)]

    def shard_body(pair_stack, mask_stack, norm_gain, norm_bias, w_proj, w_gate, hid_gain, hid_bias, w_out):
        n_crops, rows, n_res, ch = pair_stack.shape
        dev = lax.axis_index('dap')
        side = jnp.reshape(dev % 2, (1,)).astype(jnp.int32)
        col = lambda v: v.astype(F32).reshape(-1, 1)
        fin = [(0.5 * w_gate[u].T, 0.5 * w_out[u].T, col(hid_gain[u]), col(hid_bias[u])) for u in range(2)]
        wp = [0.5 * w_proj[u].T for u in range(2)]
        ln = [(col(norm_gain[u]), col(norm_bias[u])) for u in range(2)]
        pick = jnp.concatenate([dev * rows + jnp.arange(rows), (dev ^ 1) * rows + jnp.arange(rows)])
        sel = (pick[:, None] == jnp.arange(n_res)[None, :]).astype(BF)

        mask_all = lax.all_gather(mask_stack.astype(BF), 'dap', axis=1, tiled=True)
        mask_cols = jnp.swapaxes(lax.dynamic_slice_in_dim(mask_all, dev * rows, rows, 2), 1, 2)
        z_all = [lax.all_gather(turn(pair_stack, crop), 'dap', axis=0, tiled=True) for crop in range(n_crops)]

        projs, halves, sums = {}, {}, {}
        last = [None]

        def after_last(args):
            if last[0] is None:
                return args
            table, key = last[0]
            head, *tail = table[key]
            head, *args = lax.optimization_barrier((head, *args))
            table[key] = (head, *tail)
            return args

        def project(crop):
            z_all[crop], = after_last([z_all[crop]])
            x0, a0, b0 = proj0(side, z_all[crop], mask_all[crop], wp[0], *ln[0])
            projs[crop] = a0, b0, lax.ppermute(b0, 'dap', swap), x0
            last[0] = projs, crop

        def outgoing(crop):
            a0, b0, b0p, x0 = projs[crop]
            b0, b0p = after_last([b0, b0p])
            a0 = projs[crop][0]
            t0 = tri0(side, a0, b0, b0p)
            mine, a1 = fin0(side, t0, z_all[crop], x0, mask_all[crop], fin[0] + (wp[1][:2 * ch],) + ln[1] + (sel,))
            halves[crop] = mine, a1, lax.ppermute(a1, 'dap', swap)
            last[0] = halves, crop

        def incoming(crop):
            mine, a1, a1p = halves[crop]
            a1, a1p = after_last([a1, a1p])
            mine = halves[crop][0]
            z1, x1, b1 = proj1(side, mine, a1p, mask_cols[crop], wp[1][2 * ch:], *ln[1])
            sums[crop] = tri1(side, b1, a1, a1p), z1, x1
            last[0] = sums, crop

        lead = min(LEAD, n_crops - 1)
        steps = []
        for crop in range(lead):
            steps += [(project, crop)] + ([(incoming, crop - 1)] if crop else []) + [(outgoing, crop)]
        steps += [(project, lead)]
        for crop in range(lead, n_crops):
            steps += [(project, crop + 1)] if crop + 1 < n_crops else []
            steps += ([(incoming, crop - 1)] if crop == lead and lead else []) + [(outgoing, crop)]
            steps += [(incoming, crop - 1)] if crop > lead else []
        steps += [(incoming, n_crops - 1)]
        out = None
        for f, crop in steps:
            waiting = list(sums)
            f(crop)
            for c in waiting:
                t1, z1, x1 = sums.pop(c)
                out = fin1(t1, z1, x1, fin[1], c, n_crops, out)
        for c in list(sums):
            t1, z1, x1 = sums.pop(c)
            out = fin1(t1, z1, x1, fin[1], c, n_crops, out)
        return out

    rep = P()
    in_specs = (P('data', 'dap', None, None), P('data', 'dap', None)) + (rep,) * 7
    return jax.shard_map(shard_body, mesh=mesh, in_specs=in_specs,
                         out_specs=P('data', None, 'dap', None), check_vma=False)
```
